32 devices in a mesh: rows: 8 (over y, x, core), feat: 4 (over z).
Axes of the slice: x: 2, y: 2, z: 4, core: 2. Of those that a mesh axis runs over, the one named last changes fastest.
Arguments:
- features: bfloat16 [8192, 2048], P('rows', 'feat'), may hold values from -6 to 6
- grad_out: bfloat16 [8192, 2048], P('rows', 'feat'), may hold values from -6 to 6
- eigvecs: float32 [2048, 2048], P('feat', 'rows'), may hold values from -1 to 1, as said below
- eigvals: float32 [2048], replicated, may hold values from 0.1 to 1, as said below
- whiten: bfloat16 [2048, 2048], P(None, 'feat'), may hold values from -0.125 to 0.125
Outputs:
- grad_in: bfloat16 [8192, 2048], P('rows', 'feat')
The draws below stay inside these ranges and needn't reach their ends.
Inputs may be any that keep to these rules, and one draw needn't show every extreme that they name: `eigvecs`: the columns are orthonormal. `eigvals`: any two entries differ by at least 0.45 / 2048.
All inputs are finite; a program needn't handle non-finite values.
Results may differ from the reference program's by a relative error of at most 0.0074.
Values may be sent and summed in bfloat16 or wider, within the bound.
A program may use at most 128 MiB of HBM per device.

```python
import jax
import jax.numpy as jnp
from jax import lax

D = 2048
TOKENS = 8192


def draw_eigvecs(key, part):
    normal_mat = jax.random.normal(key, (D, D), jnp.float32)
    ortho, upper = jnp.linalg.qr(normal_mat)
    return ortho


def draw_eigvals(key, part):
    ranking = jax.random.permutation(jax.random.fold_in(key, 1), D)
    jitter = jax.random.uniform(jax.random.fold_in(key, 2), (D,), jnp.float32)
    return 0.1 + 0.9 * (ranking.astype(jnp.float32) + 0.25 + 0.5 * jitter) / D


def block_levels(own_key, extent, shards, low, top_value):
    loudness, own = 1.0, jax.random.fold_in(own_key, 6)
    for dim, parts in shards:
        heights = jnp.exp(jax.random.uniform(jax.random.fold_in(own, dim), (parts,), jnp.float32, low / len(shards), top_value / len(shards)))
        loudness = loudness * jnp.repeat(heights, extent[dim] // parts).reshape([-1 if axis == dim else 1 for axis in range(len(extent))])
    return loudness


def gaussian(own_key, extent, width, bound, split=(), held_as=jnp.bfloat16):
    entries = width * jax.random.normal(own_key, extent, jnp.float32)
    if split:
        entries = entries * block_levels(own_key, extent, split, -0.22, 0.18)
    return jnp.clip(entries, -bound, bound).astype(held_as)


def setup_inputs(seed: int = 0) -> dict:
    keys = jax.random.split(jax.random.key(seed), 6)
    return {
        "features": gaussian(keys[0], (TOKENS, D), 1.0, 6.0, ((0, 8), (1, 4))),
        "grad_out": gaussian(keys[1], (TOKENS, D), 1.0, 6.0, ((0, 8), (1, 4))),
        "eigvecs": draw_eigvecs(jax.random.fold_in(keys[5], 71), 0),
        "eigvals": draw_eigvals(jax.random.fold_in(keys[5], 71), 0),
        "whiten": gaussian(keys[4], (D, D), D ** -0.5, 0.125, ((1, 4),)),
    }


def divided(lam_row, lam_col, first_col):
    on_diag = jnp.arange(lam_row.shape[0], dtype=jnp.int32)[:, None] == (first_col + jnp.arange(lam_col.shape[0], dtype=jnp.int32))[None, :]
    root_row = lam_row ** (-0.5)
    root_col = lam_col ** (-0.5)
    gaps_lam = lam_row[:, None] - lam_col[None, :]
    safe_gap = jnp.where(on_diag, jnp.ones_like(gaps_lam), gaps_lam)
    off_diag = (root_row[:, None] - root_col[None, :]) / safe_gap
    diag_vals = -0.5 * lam_row[:, None] ** (-1.5) + jnp.zeros_like(gaps_lam)
    return jnp.where(on_diag, diag_vals, off_diag)

def reference(features, grad_out, eigvecs, eigvals, whiten):
    highest = lax.Precision.HIGHEST
    row_count = features.shape[0]
    col_mean = jnp.sum(features.astype(jnp.float32), axis=0) / row_count
    grad_mean = jnp.sum(grad_out.astype(jnp.float32), axis=0) / row_count
    cross_prod = jnp.dot(features.T.astype(jnp.float32), grad_out.astype(jnp.float32), preferred_element_type=jnp.float32) - row_count * jnp.outer(col_mean, grad_mean)
    sym_gram = 0.5 * (cross_prod + cross_prod.T)
    rotated = jnp.dot(eigvecs.T, jnp.dot(sym_gram, eigvecs, precision=highest), precision=highest)
    kernel = divided(eigvals, eigvals, 0)
    sens = jnp.dot(jnp.dot(eigvecs, kernel * rotated, precision=highest), eigvecs.T, precision=highest)
    sens_scaled = (2.0 / row_count * sens).astype(jnp.bfloat16)
    shifted = (grad_out.astype(jnp.float32) - grad_mean).astype(jnp.bfloat16)
    centered = (features.astype(jnp.float32) - col_mean).astype(jnp.bfloat16)
    grad_in = jnp.dot(shifted.astype(jnp.float32), whiten.astype(jnp.float32), preferred_element_type=jnp.float32) + jnp.dot(centered.astype(jnp.float32), sens_scaled.T.astype(jnp.float32), preferred_element_type=jnp.float32)
    return grad_in.astype(jnp.bfloat16)
```

```python
import functools

import jax
import jax.numpy as jnp
from jax import lax
from jax.experimental import pallas as pl
from jax.experimental.pallas import tpu as pltpu
from jax.sharding import PartitionSpec as P

MESH = pl.DeviceIdType.MESH
VMEM = pl.BlockSpec(memory_space=pltpu.VMEM)
bf16, f32 = jnp.bfloat16, jnp.float32


def peer(axis, index):
    return {axis: index}


def greet(axis, targets):
    barrier = pltpu.get_barrier_semaphore()
    for target in targets:
        pl.semaphore_signal(barrier, inc=1, device_id=peer(axis, target), device_id_type=MESH)
    pl.semaphore_wait(barrier, len(targets))


def remote(src, dst, send, recv, axis, target):
    return pltpu.make_async_remote_copy(
        src_ref=src, dst_ref=dst, send_sem=send, recv_sem=recv,
        device_id=peer(axis, target), device_id_type=MESH,
    )


def exchange_kernel(axis, n, same, x_ref, o_ref, send, recv):
    me = lax.axis_index(axis)
    targets = [lax.rem(me + d, n) for d in range(1, n)]
    greet(axis, targets)
    copies = []
    for d in range(1, n):
        src = x_ref if same else x_ref.at[targets[d - 1]]
        copy = remote(src, o_ref.at[me], send.at[d - 1], recv.at[d - 1], axis, targets[d - 1])
        copy.start()
        copies.append(copy)
    o_ref[me] = x_ref[...] if same else x_ref[me]
    for copy in copies:
        copy.wait()


def gather_kernel(axis, n, x_ref, o_ref, send, recv, core_send, core_recv):
    me = lax.axis_index(axis)
    core = lax.rem(me, 2)
    mate = me + 1 - 2 * core
    h = n // 2
    targets = [lax.rem(me + 2 * d, n) for d in range(1, h)]
    greet(axis, [mate] + targets)
    copies = []
    for d in range(1, h):
        copy = remote(x_ref, o_ref.at[me], send.at[d], recv.at[d], axis, targets[d - 1])
        copy.start()
        copies.append(copy)
    passed = [remote(x_ref, o_ref.at[me], core_send.at[0], core_recv.at[0], axis, mate)]
    passed[0].start()
    o_ref[me] = x_ref[...]
    for d in range(1, h):
        source = lax.rem(me + n - 2 * d, n)
        copies[d - 1].wait_recv()
        copy = remote(o_ref.at[source], o_ref.at[source], core_send.at[d], core_recv.at[d], axis, mate)
        copy.start()
        passed.append(copy)
    for copy in copies:
        copy.wait_send()
    for copy in passed:
        copy.wait()


def scatter_kernel(axis, n, x_ref, o_ref, landed, stage, parts, send, recv, core_send, core_recv):
    me = lax.axis_index(axis)
    core = lax.rem(me, 2)
    chip = me // 2
    mate = me + 1 - 2 * core
    h = n // 2
    targets = [lax.rem(me + 2 * d, n) for d in range(1, h)]
    greet(axis, [mate] + targets)
    core_copies = []
    for d in list(range(1, h)) + [0]:
        there = lax.rem(chip + d, h)
        copy = remote(x_ref.at[1 - core, there], landed.at[d], core_send.at[d], core_recv.at[d], axis, mate)
        copy.start()
        core_copies.append(copy)
    copies = []
    for order, d in enumerate(range(1, h)):
        there = lax.rem(chip + d, h)
        core_copies[order].wait_recv()
        stage[d - 1] = (x_ref[core, there].astype(f32) + landed[d].astype(f32)).astype(bf16)
        copy = remote(stage.at[d - 1], parts.at[d - 1], send.at[d - 1], recv.at[d - 1], axis, targets[d - 1])
        copy.start()
        copies.append(copy)
    core_copies[-1].wait_recv()
    total = x_ref[core, chip].astype(f32) + landed[0].astype(f32)
    for d in range(1, h):
        copies[d - 1].wait_recv()
        total = total + parts[d - 1].astype(f32)
    o_ref[...] = total.astype(bf16)
    for copy in copies + core_copies:
        copy.wait_send()


def call(kernel, out, scratch, cid, sent, *args):
    return pl.pallas_call(
        kernel,
        out_shape=out,
        in_specs=[VMEM] * len(args),
        out_specs=VMEM,
        scratch_shapes=scratch,
        compiler_params=pltpu.CompilerParams(collective_id=cid, has_side_effects=True, vmem_limit_bytes=48 * 2**20),
        cost_estimate=pl.CostEstimate(flops=8_000_000_000, bytes_accessed=sent, transcendentals=0),
    )(*args)


def exchange(x, axis, cid, same=False):
    n = lax.axis_size(axis)
    shape = (n,) + x.shape if same else x.shape
    sems = [pltpu.SemaphoreType.DMA((n - 1,))] * 2
    return call(functools.partial(exchange_kernel, axis, n, same), jax.ShapeDtypeStruct(shape, x.dtype), sems, cid, x.nbytes, x)


def gather(x, axis, cid):
    n = lax.axis_size(axis)
    sems = [pltpu.SemaphoreType.DMA((n // 2,))] * 4
    return call(functools.partial(gather_kernel, axis, n), jax.ShapeDtypeStruct((n,) + x.shape, x.dtype), sems, cid, x.nbytes, x)


def scatter(x, axis, cid):
    n = lax.axis_size(axis)
    h, piece = n // 2, x.shape[2:]
    scratch = [pltpu.VMEM((h,) + piece, bf16), pltpu.VMEM((h,) + piece, bf16), pltpu.VMEM((h,) + piece, bf16)]
    scratch += [pltpu.SemaphoreType.DMA((h,))] * 4
    return call(functools.partial(scatter_kernel, axis, n), jax.ShapeDtypeStruct(piece, bf16), scratch, cid, x.nbytes, x)


def divided(lam_row, lam_col, first_row):
    on_diag = (
        (first_row + jnp.arange(lam_row.shape[0], dtype=jnp.int32))[:, None]
        == jnp.arange(lam_col.shape[0], dtype=jnp.int32)[None, :]
    )
    root_row = lam_row ** (-0.5)
    root_col = lam_col ** (-0.5)
    gaps_lam = lam_row[:, None] - lam_col[None, :]
    safe_gap = jnp.where(on_diag, jnp.ones_like(gaps_lam), gaps_lam)
    off_diag = (root_row[:, None] - root_col[None, :]) / safe_gap
    diag_vals = -0.5 * lam_row[:, None] ** (-1.5) + jnp.zeros_like(gaps_lam)
    return jnp.where(on_diag, diag_vals, off_diag)


def dot(a, b, ca, cb):
    return lax.dot_general(a, b, (((ca,), (cb,)), ((), ())), preferred_element_type=f32)


def local(features, grad_out, eigvecs, eigvals, whiten):
    tok_rows, own = features.shape
    n = lax.axis_size("rows")
    d_all = eigvals.shape[0]
    nar = d_all // n
    row_count = tok_rows * n
    me = lax.axis_index("rows")

    v_col = lax.all_gather(eigvecs.astype(bf16), "feat", axis=0, tiled=True)
    sums = jnp.stack([jnp.sum(features, axis=0, dtype=f32), jnp.sum(grad_out, axis=0, dtype=f32)])
    sums = jnp.pad(sums, ((0, 6), (0, 0)))
    means = jnp.sum(gather(sums, "rows", 1), axis=0) / row_count
    xc = (features.astype(f32) - means[0]).astype(bf16)
    gc = (grad_out.astype(f32) - means[1]).astype(bf16)
    g_all = lax.all_gather(gc, "feat", axis=1, tiled=True)
    v_all = gather(v_col, "rows", 2).transpose(1, 0, 2).reshape(d_all, d_all)

    xc, g_all = lax.optimization_barrier((xc, g_all))
    x_all = lax.all_gather(xc, "feat", axis=1, tiled=True)
    part = dot(xc, g_all, 0, 0).astype(bf16)
    part = part.reshape(own, n // 2, 2, nar).transpose(2, 1, 0, 3)
    tile = scatter(part, "rows", 3)
    c_col = exchange(tile, "feat", 4, same=True).reshape(n, nar, nar)
    turned = exchange(c_col, "rows", 5)
    both = 0.5 * (c_col.astype(f32) + turned.transpose(0, 2, 1).astype(f32))
    both = both.reshape(d_all, nar).astype(bf16)
    half = dot(v_all, both, 0, 0).astype(bf16)
    half = exchange(half.reshape(n, nar, nar), "rows", 6)
    rotated = dot(half.transpose(1, 0, 2).reshape(nar, d_all), v_all, 1, 0)
    first = me * nar
    lam_row = lax.dynamic_slice_in_dim(eigvals, first, nar)
    scaled = (divided(lam_row, eigvals, first) * rotated).astype(bf16)
    back = dot(scaled, v_all, 1, 1).astype(bf16)
    back = exchange(back.reshape(nar, n, nar).transpose(1, 0, 2), "rows", 7).reshape(d_all, nar)
    v_own = lax.dynamic_slice_in_dim(v_all, lax.axis_index("feat") * own, own)
    sens = (2.0 / row_count * dot(v_own, back, 1, 0)).astype(bf16)
    sens = gather(sens, "rows", 8).transpose(1, 0, 2).reshape(own, d_all)
    grad_in = dot(g_all, whiten, 1, 0) + dot(x_all, sens, 1, 1)
    return grad_in.astype(bf16)


def solution(mesh):
    in_specs = (P("rows", "feat"), P("rows", "feat"), P("feat", "rows"), P(), P(None, "feat"))
    out_specs = P("rows", "feat")
    return jax.shard_map(local, mesh=mesh, in_specs=in_specs, out_specs=out_specs, check_vma=False)
```

```python
import functools

import jax
import jax.numpy as jnp
from jax import lax
from jax.experimental import pallas as pl
from jax.experimental.pallas import tpu as pltpu
from jax.sharding import PartitionSpec as P

MESH = pl.DeviceIdType.MESH
VMEM = pl.BlockSpec(memory_space=pltpu.VMEM)
bf16, f32 = jnp.bfloat16, jnp.float32


def peer(axis, index):
    return {axis: index}


def greet(axis, targets):
    barrier = pltpu.get_barrier_semaphore()
    for target in targets:
        pl.semaphore_signal(barrier, inc=1, device_id=peer(axis, target), device_id_type=MESH)
    pl.semaphore_wait(barrier, len(targets))


def remote(src, dst, send, recv, axis, target):
    return pltpu.make_async_remote_copy(
        src_ref=src, dst_ref=dst, send_sem=send, recv_sem=recv,
        device_id=peer(axis, target), device_id_type=MESH,
    )


def exchange_kernel(axis, n, same, x_ref, o_ref, send, recv):
    me = lax.axis_index(axis)
    targets = [lax.rem(me + d, n) for d in range(1, n)]
    greet(axis, targets)
    copies = []
    for d in range(1, n):
        src = x_ref if same else x_ref.at[targets[d - 1]]
        copy = remote(src, o_ref.at[me], send.at[d - 1], recv.at[d - 1], axis, targets[d - 1])
        copy.start()
        copies.append(copy)
    o_ref[me] = x_ref[...] if same else x_ref[me]
    for copy in copies:
        copy.wait()


def gather_kernel(axis, n, x_ref, o_ref, send, recv, core_send, core_recv):
    me = lax.axis_index(axis)
    core = lax.rem(me, 2)
    mate = me + 1 - 2 * core
    h = n // 2
    targets = [lax.rem(me + 2 * d, n) for d in range(1, h)]
    greet(axis, [mate] + targets)
    copies = []
    for d in range(1, h):
        copy = remote(x_ref, o_ref.at[me], send.at[d], recv.at[d], axis, targets[d - 1])
        copy.start()
        copies.append(copy)
    passed = [remote(x_ref, o_ref.at[me], core_send.at[0], core_recv.at[0], axis, mate)]
    passed[0].start()
    o_ref[me] = x_ref[...]
    for d in range(1, h):
        source = lax.rem(me + n - 2 * d, n)
        copies[d - 1].wait_recv()
        copy = remote(o_ref.at[source], o_ref.at[source], core_send.at[d], core_recv.at[d], axis, mate)
        copy.start()
        passed.append(copy)
    for copy in copies:
        copy.wait_send()
    for copy in passed:
        copy.wait()


def scatter_kernel(axis, n, x_ref, o_ref, landed, stage, parts, send, recv, core_send, core_recv):
    me = lax.axis_index(axis)
    core = lax.rem(me, 2)
    chip = me // 2
    mate = me + 1 - 2 * core
    h = n // 2
    targets = [lax.rem(me + 2 * d, n) for d in range(1, h)]
    greet(axis, [mate] + targets)
    core_copies = []
    for d in list(range(1, h)) + [0]:
        there = lax.rem(chip + d, h)
        copy = remote(x_ref.at[1 - core, there], landed.at[d], core_send.at[d], core_recv.at[d], axis, mate)
        copy.start()
        core_copies.append(copy)
    copies = []
    for order, d in enumerate(range(1, h)):
        there = lax.rem(chip + d, h)
        core_copies[order].wait_recv()
        stage[d - 1] = (x_ref[core, there].astype(f32) + landed[d].astype(f32)).astype(bf16)
        copy = remote(stage.at[d - 1], parts.at[d - 1], send.at[d - 1], recv.at[d - 1], axis, targets[d - 1])
        copy.start()
        copies.append(copy)
    core_copies[-1].wait_recv()
    total = x_ref[core, chip].astype(f32) + landed[0].astype(f32)
    for d in range(1, h):
        copies[d - 1].wait_recv()
        total = total + parts[d - 1].astype(f32)
    o_ref[...] = total.astype(bf16)
    for copy in copies + core_copies:
        copy.wait_send()


def call(kernel, out, scratch, cid, sent, *args):
    return pl.pallas_call(
        kernel,
        out_shape=out,
        in_specs=[VMEM] * len(args),
        out_specs=VMEM,
        scratch_shapes=scratch,
        compiler_params=pltpu.CompilerParams(collective_id=cid, has_side_effects=True, vmem_limit_bytes=48 * 2**20),
        cost_estimate=pl.CostEstimate(flops=8_000_000_000, bytes_accessed=sent, transcendentals=0),
    )(*args)


def exchange(x, axis, cid, same=False):
    n = lax.axis_size(axis)
    shape = (n,) + x.shape if same else x.shape
    sems = [pltpu.SemaphoreType.DMA((n - 1,))] * 2
    return call(functools.partial(exchange_kernel, axis, n, same), jax.ShapeDtypeStruct(shape, x.dtype), sems, cid, x.nbytes, x)


def gather(x, axis, cid):
    n = lax.axis_size(axis)
    sems = [pltpu.SemaphoreType.DMA((n // 2,))] * 4
    return call(functools.partial(gather_kernel, axis, n), jax.ShapeDtypeStruct((n,) + x.shape, x.dtype), sems, cid, x.nbytes, x)


def scatter(x, axis, cid):
    n = lax.axis_size(axis)
    h, piece = n // 2, x.shape[2:]
    scratch = [pltpu.VMEM((h,) + piece, bf16), pltpu.VMEM((h,) + piece, bf16), pltpu.VMEM((h,) + piece, bf16)]
    scratch += [pltpu.SemaphoreType.DMA((h,))] * 4
    return call(functools.partial(scatter_kernel, axis, n), jax.ShapeDtypeStruct(piece, bf16), scratch, cid, x.nbytes, x)


def lanes(index, width):
    return pl.ds(pl.multiple_of(index * width, width), width)


def chain_kernel(n, zn, scale, x_ref, v_ref, k_ref, o_ref, landed, stage, parts, c_col, turned, rows,
                 t_out, t_in, spread, n_out, n_in, own_q, rs, zs, ss, ts, ns, gs):
    me, z = lax.axis_index("rows"), lax.axis_index("feat")
    core, chip = lax.rem(me, 2), me // 2
    mate = me + 1 - 2 * core
    h, per = n // 2, n // zn
    nar = t_out.shape[1]
    own = x_ref.shape[0]
    barrier = pltpu.get_barrier_semaphore()
    for d in range(1, n):
        pl.semaphore_signal(barrier, inc=1, device_id={"rows": lax.rem(me + d, n)}, device_id_type=MESH)
    for d in range(1, zn):
        pl.semaphore_signal(barrier, inc=1, device_id={"feat": lax.rem(z + d, zn)}, device_id_type=MESH)
    pl.semaphore_wait(barrier, n + zn - 2)

    pending = []
    core_copies = []
    order = list(range(1, h)) + [0]
    for d in order:
        piece = 2 * lax.rem(chip + d, h) + 1 - core
        copy = remote(x_ref.at[:, lanes(piece, nar)], landed.at[d], rs[0].at[d], rs[1].at[d], "rows", mate)
        copy.start()
        core_copies.append(copy)
    copies = []
    for i, d in enumerate(order):
        piece = 2 * lax.rem(chip + d, h) + core
        core_copies[i].wait_recv()
        both = x_ref[:, lanes(piece, nar)].astype(f32) + landed[d].astype(f32)
        if d:
            stage[d] = both.astype(bf16)
            copy = remote(stage.at[d], parts.at[d], rs[2].at[d], rs[3].at[d], "rows", lax.rem(me + 2 * d, n))
            copy.start()
            copies.append(copy)
    for d in range(1, h):
        copies[d - 1].wait_recv()
        both = both + parts[d].astype(f32)
    c_col[z] = both.astype(bf16)
    pending += core_copies + copies

    def pass_tiles(block):
        for i in range(per):
            s = block * per + i
            off = lax.rem(s - me + n, n)

            @pl.when(off != 0)
            def _():
                remote(c_col.at[block, pl.ds(i * nar, nar)], turned.at[me], ss[0].at[off - 1], ss[1].at[off - 1], "rows", s).start()

            @pl.when(off == 0)
            def _():
                turned[me] = c_col[block, pl.ds(i * nar, nar)]

    z_copies = []
    for d in range(1, zn):
        copy = remote(c_col.at[z], c_col.at[z], zs[0].at[d - 1], zs[1].at[d - 1], "feat", lax.rem(z + d, zn))
        copy.start()
        z_copies.append(copy)
    pass_tiles(z)
    for d in range(1, zn):
        z_copies[d - 1].wait_recv()
        pass_tiles(lax.rem(z + zn - d, zn))
    pending += z_copies

    def add_rows(source):
        inner = c_col[source // per, pl.ds(pl.multiple_of(lax.rem(source, per) * nar, nar), nar)]
        both = 0.5 * (turned[source].astype(f32) + inner.astype(f32).T)
        rows[:, lanes(source, nar)] = both.astype(bf16)

    for d in range(n):
        source = lax.rem(me + n - d, n)
        if d:
            copy = remote(c_col.at[0, pl.ds(0, nar)], turned.at[source], ss[0].at[d - 1], ss[1].at[d - 1], "rows", lax.rem(me + d, n))
            copy.wait_recv()
            pending.append(copy)
        add_rows(source)

    def swap(make, outs, ins, sems):
        copies = []
        for d in list(range(1, n)) + [0]:
            s = lax.rem(me + d, n)
            piece = make(s).astype(bf16)
            if d:
                outs[s] = piece
                copy = remote(outs.at[s], ins.at[me], sems[0].at[d - 1], sems[1].at[d - 1], "rows", s)
                copy.start()
                copies.append(copy)
            else:
                ins[me] = piece
        return copies

    t_copies = swap(lambda s: jnp.dot(rows[...], v_ref[s], preferred_element_type=f32), t_out, t_in, ts)
    for d in range(n):
        source = lax.rem(me + n - d, n)
        if d:
            t_copies[d - 1].wait_recv()
        spread[:, lanes(source, nar)] = t_in[source].astype(f32).T.astype(bf16)
    pending += t_copies
    for q in range(n):
        block = jnp.dot(spread[...], v_ref[q], preferred_element_type=f32)
        rows[:, pl.ds(q * nar, nar)] = (k_ref[:, pl.ds(q * nar, nar)] * block).astype(bf16)

    def back(s):
        total = None
        for q in range(n):
            term = lax.dot_general(
                rows[:, pl.ds(q * nar, nar)], v_ref[q, pl.ds(pl.multiple_of(s * nar, nar), nar)],
                (((1,), (1,)), ((), ())), preferred_element_type=f32,
            )
            total = term if total is None else total + term
        return total

    n_copies = swap(back, n_out, n_in, ns)
    pending += n_copies
    total = None
    for d in range(n):
        source = lax.rem(me + n - d, n)
        if d:
            n_copies[d - 1].wait_recv()
        left = v_ref[source, pl.ds(pl.multiple_of(z * own, own), own)]
        term = jnp.dot(left, n_in[source], preferred_element_type=f32)
        total = term if total is None else total + term
    own_q[...] = (scale * total).astype(bf16)

    copies, passed = [], []
    mine = o_ref.at[:, lanes(me, nar)]
    for d in range(1, h):
        copy = remote(own_q, mine, gs[0].at[d], gs[1].at[d], "rows", lax.rem(me + 2 * d, n))
        copy.start()
        copies.append(copy)
    passed.append(remote(own_q, mine, gs[2].at[0], gs[3].at[0], "rows", mate))
    passed[0].start()
    o_ref[:, lanes(me, nar)] = own_q[...]
    for d in range(1, h):
        there = o_ref.at[:, lanes(lax.rem(me + n - 2 * d, n), nar)]
        copies[d - 1].wait_recv()
        copy = remote(there, there, gs[2].at[d], gs[3].at[d], "rows", mate)
        copy.start()
        passed.append(copy)
    for copy in passed:
        copy.wait()
    for copy in copies + pending:
        copy.wait_send()


def chain(part, v_pieces, kernel_rows, row_count):
    n, zn = lax.axis_size("rows"), lax.axis_size("feat")
    own, d_all = part.shape
    nar, h = d_all // n, n // 2
    tile, square = (h, own, nar), (n, nar, nar)
    dma = pltpu.SemaphoreType.DMA
    scratch = [pltpu.VMEM(tile, bf16)] * 3 + [pltpu.VMEM((zn, own, nar), bf16), pltpu.VMEM(square, bf16)]
    scratch += [pltpu.VMEM((nar, d_all), bf16), pltpu.VMEM(square, bf16), pltpu.VMEM(square, bf16)]
    scratch += [pltpu.VMEM((nar, d_all), bf16), pltpu.VMEM(square, bf16), pltpu.VMEM(square, bf16)]
    scratch += [pltpu.VMEM((own, nar), bf16)]
    scratch += [[dma((h,))] * 4, [dma((zn - 1,))] * 2, [dma((n - 1,))] * 2, [dma((n - 1,))] * 2]
    scratch += [[dma((n - 1,))] * 2, [dma((h,))] * 4]
    kernel = functools.partial(chain_kernel, n, zn, 2.0 / row_count)
    return call(kernel, jax.ShapeDtypeStruct((own, d_all), bf16), scratch, 9, 8 * part.nbytes, part, v_pieces, kernel_rows)


def divided(lam_row, lam_col, first_row):
    on_diag = (
        (first_row + jnp.arange(lam_row.shape[0], dtype=jnp.int32))[:, None]
        == jnp.arange(lam_col.shape[0], dtype=jnp.int32)[None, :]
    )
    root_row = lam_row ** (-0.5)
    root_col = lam_col ** (-0.5)
    gaps_lam = lam_row[:, None] - lam_col[None, :]
    safe_gap = jnp.where(on_diag, jnp.ones_like(gaps_lam), gaps_lam)
    off_diag = (root_row[:, None] - root_col[None, :]) / safe_gap
    diag_vals = -0.5 * lam_row[:, None] ** (-1.5) + jnp.zeros_like(gaps_lam)
    return jnp.where(on_diag, diag_vals, off_diag)


def dot(a, b, ca, cb):
    return lax.dot_general(a, b, (((ca,), (cb,)), ((), ())), preferred_element_type=f32)


def chain_by_calls(part, v_pieces, kernel_rows, row_count):
    n = lax.axis_size("rows")
    own, d_all = part.shape
    nar = d_all // n
    v_all = v_pieces.transpose(1, 0, 2).reshape(d_all, d_all)
    part = part.reshape(own, n // 2, 2, nar).transpose(2, 1, 0, 3)
    tile = scatter(part, "rows", 3)
    c_col = exchange(tile, "feat", 4, same=True).reshape(n, nar, nar)
    turned = exchange(c_col, "rows", 5)
    both = 0.5 * (c_col.astype(f32) + turned.transpose(0, 2, 1).astype(f32))
    half = dot(v_all, both.reshape(d_all, nar).astype(bf16), 0, 0).astype(bf16)
    half = exchange(half.reshape(n, nar, nar), "rows", 6)
    rotated = dot(half.transpose(1, 0, 2).reshape(nar, d_all), v_all, 1, 0)
    back = dot((kernel_rows * rotated).astype(bf16), v_all, 1, 1).astype(bf16)
    back = exchange(back.reshape(nar, n, nar).transpose(1, 0, 2), "rows", 7).reshape(d_all, nar)
    v_own = lax.dynamic_slice_in_dim(v_all, lax.axis_index("feat") * own, own)
    sens = (2.0 / row_count * dot(v_own, back, 1, 0)).astype(bf16)
    return gather(sens, "rows", 8).transpose(1, 0, 2).reshape(own, d_all)


def local(features, grad_out, eigvecs, eigvals, whiten):
    tok_rows, own = features.shape
    n = lax.axis_size("rows")
    d_all = eigvals.shape[0]
    nar = d_all // n
    row_count = tok_rows * n
    me = lax.axis_index("rows")

    v_col = lax.all_gather(eigvecs.astype(bf16), "feat", axis=0, tiled=True)
    sums = jnp.stack([jnp.sum(features, axis=0, dtype=f32), jnp.sum(grad_out, axis=0, dtype=f32)])
    sums = jnp.pad(sums, ((0, 6), (0, 0)))
    means = jnp.sum(gather(sums, "rows", 1), axis=0) / row_count
    xc = (features.astype(f32) - means[0]).astype(bf16)
    gc = (grad_out.astype(f32) - means[1]).astype(bf16)
    g_all = lax.all_gather(gc, "feat", axis=1, tiled=True)
    v_pieces = gather(v_col, "rows", 2)
    first = me * nar
    lam_row = lax.dynamic_slice_in_dim(eigvals, first, nar)
    kernel_rows = divided(lam_row, eigvals, first)
    xc, g_all = lax.optimization_barrier((xc, g_all))
    x_all = lax.all_gather(xc, "feat", axis=1, tiled=True)
    part = dot(xc, g_all, 0, 0).astype(bf16)
    if nar % 128 == 0:
        sens = chain(part, v_pieces, kernel_rows, row_count)
    else:
        sens = chain_by_calls(part, v_pieces, kernel_rows, row_count)
    grad_in = dot(g_all, whiten, 1, 0) + dot(x_all, sens, 1, 1)
    return grad_in.astype(bf16)


def solution(mesh):
    in_specs = (P("rows", "feat"), P("rows", "feat"), P("feat", "rows"), P(), P(None, "feat"))
    out_specs = P("rows", "feat")
    return jax.shard_map(local, mesh=mesh, in_specs=in_specs, out_specs=out_specs, check_vma=False)
```

```python
import functools

import jax
import jax.numpy as jnp
from jax import lax
from jax.experimental import pallas as pl
from jax.experimental.pallas import tpu as pltpu
from jax.sharding import PartitionSpec as P

MESH = pl.DeviceIdType.MESH
VMEM = pl.BlockSpec(memory_space=pltpu.VMEM)
bf16, f32 = jnp.bfloat16, jnp.float32


def peer(axis, index):
    return {axis: index}


def greet(axis, targets):
    barrier = pltpu.get_barrier_semaphore()
    for target in targets:
        pl.semaphore_signal(barrier, inc=1, device_id=peer(axis, target), device_id_type=MESH)
    pl.semaphore_wait(barrier, len(targets))


def remote(src, dst, send, recv, axis, target):
    return pltpu.make_async_remote_copy(
        src_ref=src, dst_ref=dst, send_sem=send, recv_sem=recv,
        device_id=peer(axis, target), device_id_type=MESH,
    )


def exchange_kernel(axis, n, same, x_ref, o_ref, send, recv):
    me = lax.axis_index(axis)
    targets = [lax.rem(me + d, n) for d in range(1, n)]
    greet(axis, targets)
    copies = []
    for d in range(1, n):
        src = x_ref if same else x_ref.at[targets[d - 1]]
        copy = remote(src, o_ref.at[me], send.at[d - 1], recv.at[d - 1], axis, targets[d - 1])
        copy.start()
        copies.append(copy)
    o_ref[me] = x_ref[...] if same else x_ref[me]
    for copy in copies:
        copy.wait()


def gather_kernel(axis, n, x_ref, o_ref, send, recv, core_send, core_recv):
    me = lax.axis_index(axis)
    core = lax.rem(me, 2)
    mate = me + 1 - 2 * core
    h = n // 2
    targets = [lax.rem(me + 2 * d, n) for d in range(1, h)]
    greet(axis, [mate] + targets)
    copies = []
    for d in range(1, h):
        copy = remote(x_ref, o_ref.at[me], send.at[d], recv.at[d], axis, targets[d - 1])
        copy.start()
        copies.append(copy)
    passed = [remote(x_ref, o_ref.at[me], core_send.at[0], core_recv.at[0], axis, mate)]
    passed[0].start()
    o_ref[me] = x_ref[...]
    for d in range(1, h):
        source = lax.rem(me + n - 2 * d, n)
        copies[d - 1].wait_recv()
        copy = remote(o_ref.at[source], o_ref.at[source], core_send.at[d], core_recv.at[d], axis, mate)
        copy.start()
        passed.append(copy)
    for copy in copies:
        copy.wait_send()
    for copy in passed:
        copy.wait()


def scatter_kernel(axis, n, x_ref, o_ref, landed, stage, parts, send, recv, core_send, core_recv):
    me = lax.axis_index(axis)
    core = lax.rem(me, 2)
    chip = me // 2
    mate = me + 1 - 2 * core
    h = n // 2
    targets = [lax.rem(me + 2 * d, n) for d in range(1, h)]
    greet(axis, [mate] + targets)
    core_copies = []
    for d in list(range(1, h)) + [0]:
        there = lax.rem(chip + d, h)
        copy = remote(x_ref.at[1 - core, there], landed.at[d], core_send.at[d], core_recv.at[d], axis, mate)
        copy.start()
        core_copies.append(copy)
    copies = []
    for order, d in enumerate(range(1, h)):
        there = lax.rem(chip + d, h)
        core_copies[order].wait_recv()
        stage[d - 1] = (x_ref[core, there].astype(f32) + landed[d].astype(f32)).astype(bf16)
        copy = remote(stage.at[d - 1], parts.at[d - 1], send.at[d - 1], recv.at[d - 1], axis, targets[d - 1])
        copy.start()
        copies.append(copy)
    core_copies[-1].wait_recv()
    total = x_ref[core, chip].astype(f32) + landed[0].astype(f32)
    for d in range(1, h):
        copies[d - 1].wait_recv()
        total = total + parts[d - 1].astype(f32)
    o_ref[...] = total.astype(bf16)
    for copy in copies + core_copies:
        copy.wait_send()


def call(kernel, out, scratch, cid, sent, *args):
    return pl.pallas_call(
        kernel,
        out_shape=out,
        in_specs=[VMEM] * len(args),
        out_specs=jax.tree.map(lambda _: VMEM, out),
        scratch_shapes=scratch,
        compiler_params=pltpu.CompilerParams(collective_id=cid, has_side_effects=True, vmem_limit_bytes=48 * 2**20),
        cost_estimate=pl.CostEstimate(flops=8_000_000_000, bytes_accessed=sent, transcendentals=0),
    )(*args)


def exchange(x, axis, cid, same=False):
    n = lax.axis_size(axis)
    shape = (n,) + x.shape if same else x.shape
    sems = [pltpu.SemaphoreType.DMA((n - 1,))] * 2
    return call(functools.partial(exchange_kernel, axis, n, same), jax.ShapeDtypeStruct(shape, x.dtype), sems, cid, x.nbytes, x)


def gather(x, axis, cid):
    n = lax.axis_size(axis)
    sems = [pltpu.SemaphoreType.DMA((n // 2,))] * 4
    return call(functools.partial(gather_kernel, axis, n), jax.ShapeDtypeStruct((n,) + x.shape, x.dtype), sems, cid, x.nbytes, x)


def scatter(x, axis, cid):
    n = lax.axis_size(axis)
    h, piece = n // 2, x.shape[2:]
    scratch = [pltpu.VMEM((h,) + piece, bf16), pltpu.VMEM((h,) + piece, bf16), pltpu.VMEM((h,) + piece, bf16)]
    scratch += [pltpu.SemaphoreType.DMA((h,))] * 4
    return call(functools.partial(scatter_kernel, axis, n), jax.ShapeDtypeStruct(piece, bf16), scratch, cid, x.nbytes, x)


def lanes(index, width):
    return pl.ds(pl.multiple_of(index * width, width), width)


def chain_kernel(n, zn, scale, x_ref, v_ref, k_ref, o_ref, landed, stage, parts, c_col, turned, rows,
                 t_out, t_in, spread, n_out, n_in, own_q, rs, zs, ss, ts, ns, gs):
    me, z = lax.axis_index("rows"), lax.axis_index("feat")
    core, chip = lax.rem(me, 2), me // 2
    mate = me + 1 - 2 * core
    h, per = n // 2, n // zn
    nar = t_out.shape[1]
    own = x_ref.shape[0]
    barrier = pltpu.get_barrier_semaphore()
    for d in range(1, n):
        pl.semaphore_signal(barrier, inc=1, device_id={"rows": lax.rem(me + d, n)}, device_id_type=MESH)
    for d in range(1, zn):
        pl.semaphore_signal(barrier, inc=1, device_id={"feat": lax.rem(z + d, zn)}, device_id_type=MESH)
    pl.semaphore_wait(barrier, n + zn - 2)

    pending = []
    core_copies = []
    order = list(range(1, h)) + [0]
    for d in order:
        piece = 2 * lax.rem(chip + d, h) + 1 - core
        copy = remote(x_ref.at[:, lanes(piece, nar)], landed.at[d], rs[0].at[d], rs[1].at[d], "rows", mate)
        copy.start()
        core_copies.append(copy)
    copies = []
    for i, d in enumerate(order):
        piece = 2 * lax.rem(chip + d, h) + core
        core_copies[i].wait_recv()
        both = x_ref[:, lanes(piece, nar)].astype(f32) + landed[d].astype(f32)
        if d:
            stage[d] = both.astype(bf16)
            copy = remote(stage.at[d], parts.at[d], rs[2].at[d], rs[3].at[d], "rows", lax.rem(me + 2 * d, n))
            copy.start()
            copies.append(copy)
    for d in range(1, h):
        copies[d - 1].wait_recv()
        both = both + parts[d].astype(f32)
    c_col[z] = both.astype(bf16)
    pending += core_copies + copies

    def pass_tiles(block):
        for i in range(per):
            s = block * per + i
            off = lax.rem(s - me + n, n)

            @pl.when(off != 0)
            def _():
                remote(c_col.at[block, pl.ds(i * nar, nar)], turned.at[me], ss[0].at[off - 1], ss[1].at[off - 1], "rows", s).start()

            @pl.when(off == 0)
            def _():
                turned[me] = c_col[block, pl.ds(i * nar, nar)]

    z_copies = []
    for d in range(1, zn):
        copy = remote(c_col.at[z], c_col.at[z], zs[0].at[d - 1], zs[1].at[d - 1], "feat", lax.rem(z + d, zn))
        copy.start()
        z_copies.append(copy)
    pass_tiles(z)
    for d in range(1, zn):
        z_copies[d - 1].wait_recv()
        pass_tiles(lax.rem(z + zn - d, zn))
    pending += z_copies

    def add_rows(source):
        inner = c_col[source // per, pl.ds(pl.multiple_of(lax.rem(source, per) * nar, nar), nar)]
        both = 0.5 * (turned[source].astype(f32) + inner.astype(f32).T)
        rows[:, lanes(source, nar)] = both.astype(bf16)

    for d in range(n):
        source = lax.rem(me + n - d, n)
        if d:
            copy = remote(c_col.at[0, pl.ds(0, nar)], turned.at[source], ss[0].at[d - 1], ss[1].at[d - 1], "rows", lax.rem(me + d, n))
            copy.wait_recv()
            pending.append(copy)
        add_rows(source)

    def swap(make, outs, ins, sems):
        copies = []
        for d in list(range(1, n)) + [0]:
            s = lax.rem(me + d, n)
            piece = make(s).astype(bf16)
            if d:
                outs[s] = piece
                copy = remote(outs.at[s], ins.at[me], sems[0].at[d - 1], sems[1].at[d - 1], "rows", s)
                copy.start()
                copies.append(copy)
            else:
                ins[me] = piece
        return copies

    t_copies = swap(lambda s: jnp.dot(rows[...], v_ref[s], preferred_element_type=f32), t_out, t_in, ts)
    for d in range(n):
        source = lax.rem(me + n - d, n)
        if d:
            t_copies[d - 1].wait_recv()
        spread[:, lanes(source, nar)] = t_in[source].astype(f32).T.astype(bf16)
    pending += t_copies
    for q in range(n):
        block = jnp.dot(spread[...], v_ref[q], preferred_element_type=f32)
        rows[:, pl.ds(q * nar, nar)] = (k_ref[:, pl.ds(q * nar, nar)] * block).astype(bf16)

    def back(s):
        total = None
        for q in range(n):
            term = lax.dot_general(
                rows[:, pl.ds(q * nar, nar)], v_ref[q, pl.ds(pl.multiple_of(s * nar, nar), nar)],
                (((1,), (1,)), ((), ())), preferred_element_type=f32,
            )
            total = term if total is None else total + term
        return total

    n_copies = swap(back, n_out, n_in, ns)
    pending += n_copies
    total = None
    for d in range(n):
        source = lax.rem(me + n - d, n)
        if d:
            n_copies[d - 1].wait_recv()
        left = v_ref[source, pl.ds(pl.multiple_of(z * own, own), own)]
        term = jnp.dot(left, n_in[source], preferred_element_type=f32)
        total = term if total is None else total + term
    own_q[...] = (scale * total).astype(bf16)

    copies, passed = [], []
    mine = o_ref.at[:, lanes(me, nar)]
    for d in range(1, h):
        copy = remote(own_q, mine, gs[0].at[d], gs[1].at[d], "rows", lax.rem(me + 2 * d, n))
        copy.start()
        copies.append(copy)
    passed.append(remote(own_q, mine, gs[2].at[0], gs[3].at[0], "rows", mate))
    passed[0].start()
    o_ref[:, lanes(me, nar)] = own_q[...]
    for d in range(1, h):
        there = o_ref.at[:, lanes(lax.rem(me + n - 2 * d, n), nar)]
        copies[d - 1].wait_recv()
        copy = remote(there, there, gs[2].at[d], gs[3].at[d], "rows", mate)
        copy.start()
        passed.append(copy)
    for copy in passed:
        copy.wait()
    for copy in copies + pending:
        copy.wait_send()


def chain(part, v_pieces, kernel_rows, row_count):
    n, zn = lax.axis_size("rows"), lax.axis_size("feat")
    own, d_all = part.shape
    nar, h = d_all // n, n // 2
    tile, square = (h, own, nar), (n, nar, nar)
    dma = pltpu.SemaphoreType.DMA
    scratch = [pltpu.VMEM(tile, bf16)] * 3 + [pltpu.VMEM((zn, own, nar), bf16), pltpu.VMEM(square, bf16)]
    scratch += [pltpu.VMEM((nar, d_all), bf16), pltpu.VMEM(square, bf16), pltpu.VMEM(square, bf16)]
    scratch += [pltpu.VMEM((nar, d_all), bf16), pltpu.VMEM(square, bf16), pltpu.VMEM(square, bf16)]
    scratch += [pltpu.VMEM((own, nar), bf16)]
    scratch += [[dma((h,))] * 4, [dma((zn - 1,))] * 2, [dma((n - 1,))] * 2, [dma((n - 1,))] * 2]
    scratch += [[dma((n - 1,))] * 2, [dma((h,))] * 4]
    kernel = functools.partial(chain_kernel, n, zn, 2.0 / row_count)
    return call(kernel, jax.ShapeDtypeStruct((own, d_all), bf16), scratch, 9, 8 * part.nbytes, part, v_pieces, kernel_rows)


def front_kernel(n, zn, chunks, g_ref, v_ref, g_out, v_out, send, recv, near, far, mate_send, mate_recv):
    me, z = lax.axis_index("rows"), lax.axis_index("feat")
    core = lax.rem(me, 2)
    mate = me + 1 - 2 * core
    h = n // 2
    own, ck = v_ref.shape[0], g_ref.shape[0] // chunks
    units = chunks + 1
    peers = [lax.rem(me + 2 * d, n) for d in range(1, h)]
    barrier = pltpu.get_barrier_semaphore()
    for target in [mate] + peers:
        pl.semaphore_signal(barrier, inc=1, device_id={"rows": target}, device_id_type=MESH)
    for d in range(1, zn):
        pl.semaphore_signal(barrier, inc=1, device_id={"feat": lax.rem(z + d, zn)}, device_id_type=MESH)
    pl.semaphore_wait(barrier, h + zn - 1)

    def there(block, unit):
        if unit == 0:
            return v_out.at[me, pl.ds(pl.multiple_of(block * own, own), own)]
        return g_out.at[pl.ds((unit - 1) * ck, ck), lanes(block, own)]

    def hop(way, step, unit):
        block = z - step if way == 0 else z + step
        if step == 0:
            src = v_ref if unit == 0 else g_ref.at[pl.ds((unit - 1) * ck, ck)]
        else:
            src = there(block, unit)
        target = lax.rem(z + (1 if way == 0 else zn - 1), zn)
        return remote(src, there(block, unit), send.at[way, step, unit], recv.at[way, step, unit], "feat", target)

    def held(way, step):
        return z >= step if way == 0 else z + step < zn

    def onward(way):
        return z < zn - 1 if way == 0 else z > 0

    def spread(block, d, fresh=False):
        src = v_ref if fresh else there(block, 0)
        return remote(src, there(block, 0), near.at[block, d], far.at[block, d], "rows", peers[d - 1])

    def to_mate(block, d, fresh=False):
        source = lax.rem(me + n - 2 * d, n) if d else me
        ref = v_out.at[source, pl.ds(pl.multiple_of(block * own, own), own)]
        src = v_ref if fresh else ref
        return remote(src, ref, mate_send.at[block, d], mate_recv.at[block, d], "rows", mate)

    def spread_all(block, fresh=False):
        for d in range(1, h):
            spread(block, d, fresh).start()
        to_mate(block, 0, fresh).start()

    def pass_mate(block):
        for d in range(1, h):
            spread(block, d).wait_recv()
            to_mate(block, d).start()

    def each(step, what):
        if step == 0:
            what(z)
            return
        for way in (0, 1):
            @pl.when(held(way, step))
            def _():
                what(z - step if way == 0 else z + step)

    for unit in range(units):
        for way in (0, 1):
            @pl.when(onward(way))
            def _():
                hop(way, 0, unit).start()
    spread_all(z, True)
    v_out[me, pl.ds(pl.multiple_of(z * own, own), own)] = v_ref[...]
    g_out[:, lanes(z, own)] = g_ref[...]
    for step in range(1, zn):
        for unit in range(units):
            for way in (0, 1):
                @pl.when(held(way, step))
                def _():
                    hop(way, step - 1, unit).wait_recv()
                    if step < zn - 1:
                        @pl.when(onward(way))
                        def _():
                            hop(way, step, unit).start()
                    if unit == 0:
                        spread_all(z - step if way == 0 else z + step)
        each(step - 1, pass_mate)
    each(zn - 1, pass_mate)

    def finish(block):
        for d in range(1, h):
            spread(block, d).wait_send()
        for d in range(h):
            to_mate(block, d).wait()

    for step in range(zn):
        each(step, finish)
    for step in range(zn - 1):
        for unit in range(units):
            for way in (0, 1):
                @pl.when(jnp.logical_and(held(way, step), onward(way)))
                def _():
                    hop(way, step, unit).wait_send()


def front(g, v):
    n, zn = lax.axis_size("rows"), lax.axis_size("feat")
    tok, own = g.shape
    chunks = 4
    dma = pltpu.SemaphoreType.DMA
    out = (jax.ShapeDtypeStruct((tok, own * zn), bf16), jax.ShapeDtypeStruct((n, own * zn, v.shape[1]), bf16))
    scratch = [dma((2, zn - 1, chunks + 1))] * 2 + [dma((zn, n // 2))] * 4
    kernel = functools.partial(front_kernel, n, zn, chunks)
    return call(kernel, out, scratch, 10, zn * g.nbytes, g, v)


def divided(lam_row, lam_col, first_row):
    on_diag = (
        (first_row + jnp.arange(lam_row.shape[0], dtype=jnp.int32))[:, None]
        == jnp.arange(lam_col.shape[0], dtype=jnp.int32)[None, :]
    )
    root_row = lam_row ** (-0.5)
    root_col = lam_col ** (-0.5)
    gaps_lam = lam_row[:, None] - lam_col[None, :]
    safe_gap = jnp.where(on_diag, jnp.ones_like(gaps_lam), gaps_lam)
    off_diag = (root_row[:, None] - root_col[None, :]) / safe_gap
    diag_vals = -0.5 * lam_row[:, None] ** (-1.5) + jnp.zeros_like(gaps_lam)
    return jnp.where(on_diag, diag_vals, off_diag)


def dot(a, b, ca, cb):
    return lax.dot_general(a, b, (((ca,), (cb,)), ((), ())), preferred_element_type=f32)


def chain_by_calls(part, v_pieces, kernel_rows, row_count):
    n = lax.axis_size("rows")
    own, d_all = part.shape
    nar = d_all // n
    v_all = v_pieces.transpose(1, 0, 2).reshape(d_all, d_all)
    part = part.reshape(own, n // 2, 2, nar).transpose(2, 1, 0, 3)
    tile = scatter(part, "rows", 3)
    c_col = exchange(tile, "feat", 4, same=True).reshape(n, nar, nar)
    turned = exchange(c_col, "rows", 5)
    both = 0.5 * (c_col.astype(f32) + turned.transpose(0, 2, 1).astype(f32))
    half = dot(v_all, both.reshape(d_all, nar).astype(bf16), 0, 0).astype(bf16)
    half = exchange(half.reshape(n, nar, nar), "rows", 6)
    rotated = dot(half.transpose(1, 0, 2).reshape(nar, d_all), v_all, 1, 0)
    back = dot((kernel_rows * rotated).astype(bf16), v_all, 1, 1).astype(bf16)
    back = exchange(back.reshape(nar, n, nar).transpose(1, 0, 2), "rows", 7).reshape(d_all, nar)
    v_own = lax.dynamic_slice_in_dim(v_all, lax.axis_index("feat") * own, own)
    sens = (2.0 / row_count * dot(v_own, back, 1, 0)).astype(bf16)
    return gather(sens, "rows", 8).transpose(1, 0, 2).reshape(own, d_all)


def local(features, grad_out, eigvecs, eigvals, whiten):
    tok_rows, own = features.shape
    n = lax.axis_size("rows")
    d_all = eigvals.shape[0]
    nar = d_all // n
    row_count = tok_rows * n
    me = lax.axis_index("rows")

    sums = jnp.stack([jnp.sum(features, axis=0, dtype=f32), jnp.sum(grad_out, axis=0, dtype=f32)])
    sums = jnp.pad(sums, ((0, 6), (0, 0)))
    means = jnp.sum(gather(sums, "rows", 1), axis=0) / row_count
    xc = (features.astype(f32) - means[0]).astype(bf16)
    gc = (grad_out.astype(f32) - means[1]).astype(bf16)
    g_all, v_pieces = front(gc, eigvecs.astype(bf16))
    first = me * nar
    lam_row = lax.dynamic_slice_in_dim(eigvals, first, nar)
    kernel_rows = divided(lam_row, eigvals, first)
    xc, g_all = lax.optimization_barrier((xc, g_all))
    x_all = lax.all_gather(xc, "feat", axis=1, tiled=True)
    part = dot(xc, g_all, 0, 0).astype(bf16)
    if nar % 128 == 0:
        sens = chain(part, v_pieces, kernel_rows, row_count)
    else:
        sens = chain_by_calls(part, v_pieces, kernel_rows, row_count)
    grad_in = dot(g_all, whiten, 1, 0) + dot(x_all, sens, 1, 1)
    return grad_in.astype(bf16)


def solution(mesh):
    in_specs = (P("rows", "feat"), P("rows", "feat"), P("feat", "rows"), P(), P(None, "feat"))
    out_specs = P("rows", "feat")
    return jax.shard_map(local, mesh=mesh, in_specs=in_specs, out_specs=out_specs, check_vma=False)
```

```python
import functools

import jax
import jax.numpy as jnp
from jax import lax
from jax.experimental import pallas as pl
from jax.experimental.pallas import tpu as pltpu
from jax.sharding import PartitionSpec as P

MESH = pl.DeviceIdType.MESH
VMEM = pl.BlockSpec(memory_space=pltpu.VMEM)
bf16, f32 = jnp.bfloat16, jnp.float32


def peer(axis, index):
    return {axis: index}


def greet(axis, targets):
    barrier = pltpu.get_barrier_semaphore()
    for target in targets:
        pl.semaphore_signal(barrier, inc=1, device_id=peer(axis, target), device_id_type=MESH)
    pl.semaphore_wait(barrier, len(targets))


def remote(src, dst, send, recv, axis, target):
    return pltpu.make_async_remote_copy(
        src_ref=src, dst_ref=dst, send_sem=send, recv_sem=recv,
        device_id=peer(axis, target), device_id_type=MESH,
    )


def exchange_kernel(axis, n, same, x_ref, o_ref, send, recv):
    me = lax.axis_index(axis)
    targets = [lax.rem(me + d, n) for d in range(1, n)]
    greet(axis, targets)
    copies = []
    for d in range(1, n):
        src = x_ref if same else x_ref.at[targets[d - 1]]
        copy = remote(src, o_ref.at[me], send.at[d - 1], recv.at[d - 1], axis, targets[d - 1])
        copy.start()
        copies.append(copy)
    o_ref[me] = x_ref[...] if same else x_ref[me]
    for copy in copies:
        copy.wait()


def gather_kernel(axis, n, x_ref, o_ref, send, recv, core_send, core_recv):
    me = lax.axis_index(axis)
    core = lax.rem(me, 2)
    mate = me + 1 - 2 * core
    h = n // 2
    targets = [lax.rem(me + 2 * d, n) for d in range(1, h)]
    greet(axis, [mate] + targets)
    copies = []
    for d in range(1, h):
        copy = remote(x_ref, o_ref.at[me], send.at[d], recv.at[d], axis, targets[d - 1])
        copy.start()
        copies.append(copy)
    passed = [remote(x_ref, o_ref.at[me], core_send.at[0], core_recv.at[0], axis, mate)]
    passed[0].start()
    o_ref[me] = x_ref[...]
    for d in range(1, h):
        source = lax.rem(me + n - 2 * d, n)
        copies[d - 1].wait_recv()
        copy = remote(o_ref.at[source], o_ref.at[source], core_send.at[d], core_recv.at[d], axis, mate)
        copy.start()
        passed.append(copy)
    for copy in copies:
        copy.wait_send()
    for copy in passed:
        copy.wait()


def scatter_kernel(axis, n, x_ref, o_ref, landed, stage, parts, send, recv, core_send, core_recv):
    me = lax.axis_index(axis)
    core = lax.rem(me, 2)
    chip = me // 2
    mate = me + 1 - 2 * core
    h = n // 2
    targets = [lax.rem(me + 2 * d, n) for d in range(1, h)]
    greet(axis, [mate] + targets)
    core_copies = []
    for d in list(range(1, h)) + [0]:
        there = lax.rem(chip + d, h)
        copy = remote(x_ref.at[1 - core, there], landed.at[d], core_send.at[d], core_recv.at[d], axis, mate)
        copy.start()
        core_copies.append(copy)
    copies = []
    for order, d in enumerate(range(1, h)):
        there = lax.rem(chip + d, h)
        core_copies[order].wait_recv()
        stage[d - 1] = (x_ref[core, there].astype(f32) + landed[d].astype(f32)).astype(bf16)
        copy = remote(stage.at[d - 1], parts.at[d - 1], send.at[d - 1], recv.at[d - 1], axis, targets[d - 1])
        copy.start()
        copies.append(copy)
    core_copies[-1].wait_recv()
    total = x_ref[core, chip].astype(f32) + landed[0].astype(f32)
    for d in range(1, h):
        copies[d - 1].wait_recv()
        total = total + parts[d - 1].astype(f32)
    o_ref[...] = total.astype(bf16)
    for copy in copies + core_copies:
        copy.wait_send()


def call(kernel, out, scratch, cid, sent, *args):
    return pl.pallas_call(
        kernel,
        out_shape=out,
        in_specs=[VMEM] * len(args),
        out_specs=jax.tree.map(lambda _: VMEM, out),
        scratch_shapes=scratch,
        compiler_params=pltpu.CompilerParams(collective_id=cid, has_side_effects=True, vmem_limit_bytes=48 * 2**20),
        cost_estimate=pl.CostEstimate(flops=8_000_000_000, bytes_accessed=sent, transcendentals=0),
    )(*args)


def exchange(x, axis, cid, same=False):
    n = lax.axis_size(axis)
    shape = (n,) + x.shape if same else x.shape
    sems = [pltpu.SemaphoreType.DMA((n - 1,))] * 2
    return call(functools.partial(exchange_kernel, axis, n, same), jax.ShapeDtypeStruct(shape, x.dtype), sems, cid, x.nbytes, x)


def gather(x, axis, cid):
    n = lax.axis_size(axis)
    sems = [pltpu.SemaphoreType.DMA((n // 2,))] * 4
    return call(functools.partial(gather_kernel, axis, n), jax.ShapeDtypeStruct((n,) + x.shape, x.dtype), sems, cid, x.nbytes, x)


def scatter(x, axis, cid):
    n = lax.axis_size(axis)
    h, piece = n // 2, x.shape[2:]
    scratch = [pltpu.VMEM((h,) + piece, bf16), pltpu.VMEM((h,) + piece, bf16), pltpu.VMEM((h,) + piece, bf16)]
    scratch += [pltpu.SemaphoreType.DMA((h,))] * 4
    return call(functools.partial(scatter_kernel, axis, n), jax.ShapeDtypeStruct(piece, bf16), scratch, cid, x.nbytes, x)


def lanes(index, width):
    return pl.ds(pl.multiple_of(index * width, width), width)


def chain_kernel(n, zn, chunks, scale, x_ref, v_ref, k_ref, f_ref, o_ref, f_out, landed, stage, parts, c_col, turned, rows,
                 t_out, t_in, spread, n_out, n_in, own_q, rs, zs, ss, ts, ns, gs, fs):
    me, z = lax.axis_index("rows"), lax.axis_index("feat")
    core, chip = lax.rem(me, 2), me // 2
    mate = me + 1 - 2 * core
    h, per = n // 2, n // zn
    nar = t_out.shape[1]
    own = x_ref.shape[0]
    barrier = pltpu.get_barrier_semaphore()
    for d in range(1, n):
        pl.semaphore_signal(barrier, inc=1, device_id={"rows": lax.rem(me + d, n)}, device_id_type=MESH)
    for d in range(1, zn):
        pl.semaphore_signal(barrier, inc=1, device_id={"feat": lax.rem(z + d, zn)}, device_id_type=MESH)
    pl.semaphore_wait(barrier, n + zn - 2)
    ck = f_ref.shape[0] // chunks

    def hop(way, step, unit):
        there = f_out.at[pl.ds(unit * ck, ck), lanes(z - step if way == 0 else z + step, own)]
        src = there if step else f_ref.at[pl.ds(unit * ck, ck)]
        target = lax.rem(z + (1 if way == 0 else zn - 1), zn)
        return remote(src, there, fs[0].at[way, step, unit], fs[1].at[way, step, unit], "feat", target)

    def held(way, step):
        return z >= step if way == 0 else z + step < zn

    def onward(way):
        return z < zn - 1 if way == 0 else z > 0

    def forward(step, some):
        for unit in some:
            for way in (0, 1):
                @pl.when(held(way, step))
                def _():
                    hop(way, step - 1, unit).wait_recv()
                    if step < zn - 1:
                        @pl.when(onward(way))
                        def _():
                            hop(way, step, unit).start()

    every = range(chunks)
    for unit in every:
        for way in (0, 1):
            @pl.when(onward(way))
            def _():
                hop(way, 0, unit).start()
    f_out[:, lanes(z, own)] = f_ref[...]

    pending = []
    core_copies = []
    order = list(range(1, h)) + [0]
    for d in order:
        piece = 2 * lax.rem(chip + d, h) + 1 - core
        copy = remote(x_ref.at[:, lanes(piece, nar)], landed.at[d], rs[0].at[d], rs[1].at[d], "rows", mate)
        copy.start()
        core_copies.append(copy)
    copies = []
    for i, d in enumerate(order):
        piece = 2 * lax.rem(chip + d, h) + core
        core_copies[i].wait_recv()
        both = x_ref[:, lanes(piece, nar)].astype(f32) + landed[d].astype(f32)
        if d:
            stage[d] = both.astype(bf16)
            copy = remote(stage.at[d], parts.at[d], rs[2].at[d], rs[3].at[d], "rows", lax.rem(me + 2 * d, n))
            copy.start()
            copies.append(copy)
    for d in range(1, h):
        copies[d - 1].wait_recv()
        both = both + parts[d].astype(f32)
    c_col[z] = both.astype(bf16)
    pending += core_copies + copies

    def pass_tiles(block):
        for i in range(per):
            s = block * per + i
            off = lax.rem(s - me + n, n)

            @pl.when(off != 0)
            def _():
                remote(c_col.at[block, pl.ds(i * nar, nar)], turned.at[me], ss[0].at[off - 1], ss[1].at[off - 1], "rows", s).start()

            @pl.when(off == 0)
            def _():
                turned[me] = c_col[block, pl.ds(i * nar, nar)]

    z_copies = []
    for d in range(1, zn):
        copy = remote(c_col.at[z], c_col.at[z], zs[0].at[d - 1], zs[1].at[d - 1], "feat", lax.rem(z + d, zn))
        copy.start()
        z_copies.append(copy)
    pass_tiles(z)
    for d in range(1, zn):
        z_copies[d - 1].wait_recv()
        pass_tiles(lax.rem(z + zn - d, zn))
    pending += z_copies
    forward(1, every)

    def add_rows(source):
        inner = c_col[source // per, pl.ds(pl.multiple_of(lax.rem(source, per) * nar, nar), nar)]
        both = 0.5 * (turned[source].astype(f32) + inner.astype(f32).T)
        rows[:, lanes(source, nar)] = both.astype(bf16)

    for d in range(n):
        source = lax.rem(me + n - d, n)
        if d:
            copy = remote(c_col.at[0, pl.ds(0, nar)], turned.at[source], ss[0].at[d - 1], ss[1].at[d - 1], "rows", lax.rem(me + d, n))
            copy.wait_recv()
            pending.append(copy)
        add_rows(source)

    def swap(make, outs, ins, sems):
        copies = []
        for d in list(range(1, n)) + [0]:
            s = lax.rem(me + d, n)
            piece = make(s).astype(bf16)
            if d:
                outs[s] = piece
                copy = remote(outs.at[s], ins.at[me], sems[0].at[d - 1], sems[1].at[d - 1], "rows", s)
                copy.start()
                copies.append(copy)
            else:
                ins[me] = piece
        return copies

    half = zn // 2
    for step in range(2, half):
        forward(step, every)
    t_copies = swap(lambda s: jnp.dot(rows[...], v_ref[s], preferred_element_type=f32), t_out, t_in, ts)
    for d in range(n):
        source = lax.rem(me + n - d, n)
        if d:
            t_copies[d - 1].wait_recv()
        spread[:, lanes(source, nar)] = t_in[source].astype(f32).T.astype(bf16)
    pending += t_copies
    if half > 1:
        forward(half, every[: chunks // 2])
    for q in range(n):
        block = jnp.dot(spread[...], v_ref[q], preferred_element_type=f32)
        rows[:, pl.ds(q * nar, nar)] = (k_ref[:, pl.ds(q * nar, nar)] * block).astype(bf16)

    def back(s):
        total = None
        for q in range(n):
            term = lax.dot_general(
                rows[:, pl.ds(q * nar, nar)], v_ref[q, pl.ds(pl.multiple_of(s * nar, nar), nar)],
                (((1,), (1,)), ((), ())), preferred_element_type=f32,
            )
            total = term if total is None else total + term
        return total

    n_copies = swap(back, n_out, n_in, ns)
    pending += n_copies
    if half > 1:
        forward(half, every[chunks // 2 :])
    total = None
    for d in range(n):
        source = lax.rem(me + n - d, n)
        if d:
            n_copies[d - 1].wait_recv()
        left = v_ref[source, pl.ds(pl.multiple_of(z * own, own), own)]
        term = jnp.dot(left, n_in[source], preferred_element_type=f32)
        total = term if total is None else total + term
    own_q[...] = (scale * total).astype(bf16)

    copies, passed = [], []
    mine = o_ref.at[:, lanes(me, nar)]
    for d in range(1, h):
        copy = remote(own_q, mine, gs[0].at[d], gs[1].at[d], "rows", lax.rem(me + 2 * d, n))
        copy.start()
        copies.append(copy)
    passed.append(remote(own_q, mine, gs[2].at[0], gs[3].at[0], "rows", mate))
    passed[0].start()
    o_ref[:, lanes(me, nar)] = own_q[...]
    for d in range(1, h):
        there = o_ref.at[:, lanes(lax.rem(me + n - 2 * d, n), nar)]
        copies[d - 1].wait_recv()
        copy = remote(there, there, gs[2].at[d], gs[3].at[d], "rows", mate)
        copy.start()
        passed.append(copy)
    for step in range(max(half, 1) + 1, zn):
        forward(step, every)
    for copy in passed:
        copy.wait()
    for copy in copies + pending:
        copy.wait_send()
    for step in range(zn - 1):
        for unit in every:
            for way in (0, 1):
                @pl.when(jnp.logical_and(held(way, step), onward(way)))
                def _():
                    hop(way, step, unit).wait_send()


def chain(part, v_pieces, kernel_rows, x, row_count):
    n, zn = lax.axis_size("rows"), lax.axis_size("feat")
    own, d_all = part.shape
    nar, h = d_all // n, n // 2
    tile, square = (h, own, nar), (n, nar, nar)
    dma = pltpu.SemaphoreType.DMA
    scratch = [pltpu.VMEM(tile, bf16)] * 3 + [pltpu.VMEM((zn, own, nar), bf16), pltpu.VMEM(square, bf16)]
    scratch += [pltpu.VMEM((nar, d_all), bf16), pltpu.VMEM(square, bf16), pltpu.VMEM(square, bf16)]
    scratch += [pltpu.VMEM((nar, d_all), bf16), pltpu.VMEM(square, bf16), pltpu.VMEM(square, bf16)]
    scratch += [pltpu.VMEM((own, nar), bf16)]
    scratch += [[dma((h,))] * 4, [dma((zn - 1,))] * 2, [dma((n - 1,))] * 2, [dma((n - 1,))] * 2]
    chunks = 4
    scratch += [[dma((n - 1,))] * 2, [dma((h,))] * 4, [dma((2, zn - 1, chunks))] * 2]
    kernel = functools.partial(chain_kernel, n, zn, chunks, 2.0 / row_count)
    out = (jax.ShapeDtypeStruct((own, d_all), bf16), jax.ShapeDtypeStruct((x.shape[0], own * zn), bf16))
    return call(kernel, out, scratch, 9, 8 * part.nbytes, part, v_pieces, kernel_rows, x)


def front_kernel(n, zn, chunks, g_ref, v_ref, g_out, v_out, send, recv, near, far, mate_send, mate_recv):
    me, z = lax.axis_index("rows"), lax.axis_index("feat")
    core = lax.rem(me, 2)
    mate = me + 1 - 2 * core
    h = n // 2
    own, ck = v_ref.shape[0], g_ref.shape[0] // chunks
    units = chunks + 1
    peers = [lax.rem(me + 2 * d, n) for d in range(1, h)]
    barrier = pltpu.get_barrier_semaphore()
    for target in [mate] + peers:
        pl.semaphore_signal(barrier, inc=1, device_id={"rows": target}, device_id_type=MESH)
    for d in range(1, zn):
        pl.semaphore_signal(barrier, inc=1, device_id={"feat": lax.rem(z + d, zn)}, device_id_type=MESH)
    pl.semaphore_wait(barrier, h + zn - 1)

    def there(block, unit):
        if unit == 0:
            return v_out.at[me, pl.ds(pl.multiple_of(block * own, own), own)]
        return g_out.at[pl.ds((unit - 1) * ck, ck), lanes(block, own)]

    def hop(way, step, unit):
        block = z - step if way == 0 else z + step
        if step == 0:
            src = v_ref if unit == 0 else g_ref.at[pl.ds((unit - 1) * ck, ck)]
        else:
            src = there(block, unit)
        target = lax.rem(z + (1 if way == 0 else zn - 1), zn)
        return remote(src, there(block, unit), send.at[way, step, unit], recv.at[way, step, unit], "feat", target)

    def held(way, step):
        return z >= step if way == 0 else z + step < zn

    def onward(way):
        return z < zn - 1 if way == 0 else z > 0

    def spread(block, d, fresh=False):
        src = v_ref if fresh else there(block, 0)
        return remote(src, there(block, 0), near.at[block, d], far.at[block, d], "rows", peers[d - 1])

    def to_mate(block, d, fresh=False):
        source = lax.rem(me + n - 2 * d, n) if d else me
        ref = v_out.at[source, pl.ds(pl.multiple_of(block * own, own), own)]
        src = v_ref if fresh else ref
        return remote(src, ref, mate_send.at[block, d], mate_recv.at[block, d], "rows", mate)

    def spread_all(block, fresh=False):
        for d in range(1, h):
            spread(block, d, fresh).start()
        to_mate(block, 0, fresh).start()

    def pass_mate(block):
        for d in range(1, h):
            spread(block, d).wait_recv()
            to_mate(block, d).start()

    def each(step, what):
        if step == 0:
            what(z)
            return
        for way in (0, 1):
            @pl.when(held(way, step))
            def _():
                what(z - step if way == 0 else z + step)

    for unit in range(units):
        for way in (0, 1):
            @pl.when(onward(way))
            def _():
                hop(way, 0, unit).start()
    spread_all(z, True)
    v_out[me, pl.ds(pl.multiple_of(z * own, own), own)] = v_ref[...]
    g_out[:, lanes(z, own)] = g_ref[...]
    for step in range(1, zn):
        for unit in range(units):
            for way in (0, 1):
                @pl.when(held(way, step))
                def _():
                    hop(way, step - 1, unit).wait_recv()
                    if step < zn - 1:
                        @pl.when(onward(way))
                        def _():
                            hop(way, step, unit).start()
                    if unit == 0:
                        spread_all(z - step if way == 0 else z + step)
        each(step - 1, pass_mate)
    each(zn - 1, pass_mate)

    def finish(block):
        for d in range(1, h):
            spread(block, d).wait_send()
        for d in range(h):
            to_mate(block, d).wait()

    for step in range(zn):
        each(step, finish)
    for step in range(zn - 1):
        for unit in range(units):
            for way in (0, 1):
                @pl.when(jnp.logical_and(held(way, step), onward(way)))
                def _():
                    hop(way, step, unit).wait_send()


def front(g, v):
    n, zn = lax.axis_size("rows"), lax.axis_size("feat")
    tok, own = g.shape
    chunks = 4
    dma = pltpu.SemaphoreType.DMA
    out = (jax.ShapeDtypeStruct((tok, own * zn), bf16), jax.ShapeDtypeStruct((n, own * zn, v.shape[1]), bf16))
    scratch = [dma((2, zn - 1, chunks + 1))] * 2 + [dma((zn, n // 2))] * 4
    kernel = functools.partial(front_kernel, n, zn, chunks)
    return call(kernel, out, scratch, 10, zn * g.nbytes, g, v)


def divided(lam_row, lam_col, first_row):
    on_diag = (
        (first_row + jnp.arange(lam_row.shape[0], dtype=jnp.int32))[:, None]
        == jnp.arange(lam_col.shape[0], dtype=jnp.int32)[None, :]
    )
    root_row = lam_row ** (-0.5)
    root_col = lam_col ** (-0.5)
    gaps_lam = lam_row[:, None] - lam_col[None, :]
    safe_gap = jnp.where(on_diag, jnp.ones_like(gaps_lam), gaps_lam)
    off_diag = (root_row[:, None] - root_col[None, :]) / safe_gap
    diag_vals = -0.5 * lam_row[:, None] ** (-1.5) + jnp.zeros_like(gaps_lam)
    return jnp.where(on_diag, diag_vals, off_diag)


def dot(a, b, ca, cb):
    return lax.dot_general(a, b, (((ca,), (cb,)), ((), ())), preferred_element_type=f32)


def chain_by_calls(part, v_pieces, kernel_rows, row_count):
    n = lax.axis_size("rows")
    own, d_all = part.shape
    nar = d_all // n
    v_all = v_pieces.transpose(1, 0, 2).reshape(d_all, d_all)
    part = part.reshape(own, n // 2, 2, nar).transpose(2, 1, 0, 3)
    tile = scatter(part, "rows", 3)
    c_col = exchange(tile, "feat", 4, same=True).reshape(n, nar, nar)
    turned = exchange(c_col, "rows", 5)
    both = 0.5 * (c_col.astype(f32) + turned.transpose(0, 2, 1).astype(f32))
    half = dot(v_all, both.reshape(d_all, nar).astype(bf16), 0, 0).astype(bf16)
    half = exchange(half.reshape(n, nar, nar), "rows", 6)
    rotated = dot(half.transpose(1, 0, 2).reshape(nar, d_all), v_all, 1, 0)
    back = dot((kernel_rows * rotated).astype(bf16), v_all, 1, 1).astype(bf16)
    back = exchange(back.reshape(nar, n, nar).transpose(1, 0, 2), "rows", 7).reshape(d_all, nar)
    v_own = lax.dynamic_slice_in_dim(v_all, lax.axis_index("feat") * own, own)
    sens = (2.0 / row_count * dot(v_own, back, 1, 0)).astype(bf16)
    return gather(sens, "rows", 8).transpose(1, 0, 2).reshape(own, d_all)


def local(features, grad_out, eigvecs, eigvals, whiten):
    tok_rows, own = features.shape
    n = lax.axis_size("rows")
    d_all = eigvals.shape[0]
    nar = d_all // n
    row_count = tok_rows * n
    me = lax.axis_index("rows")

    sums = jnp.stack([jnp.sum(features, axis=0, dtype=f32), jnp.sum(grad_out, axis=0, dtype=f32)])
    sums = jnp.pad(sums, ((0, 6), (0, 0)))
    means = jnp.sum(gather(sums, "rows", 1), axis=0) / row_count
    xc = (features.astype(f32) - means[0]).astype(bf16)
    gc = (grad_out.astype(f32) - means[1]).astype(bf16)
    g_all, v_pieces = front(gc, eigvecs.astype(bf16))
    first = me * nar
    lam_row = lax.dynamic_slice_in_dim(eigvals, first, nar)
    kernel_rows = divided(lam_row, eigvals, first)
    part = dot(xc, g_all, 0, 0).astype(bf16)
    if nar % 128 == 0:
        sens, x_all = chain(part, v_pieces, kernel_rows, xc, row_count)
    else:
        x_all = lax.all_gather(xc, "feat", axis=1, tiled=True)
        sens = chain_by_calls(part, v_pieces, kernel_rows, row_count)
    grad_in = dot(g_all, whiten, 1, 0) + dot(x_all, sens, 1, 1)
    return grad_in.astype(bf16)


def solution(mesh):
    in_specs = (P("rows", "feat"), P("rows", "feat"), P("feat", "rows"), P(), P(None, "feat"))
    out_specs = P("rows", "feat")
    return jax.shard_map(local, mesh=mesh, in_specs=in_specs, out_specs=out_specs, check_vma=False)
```

```python
import functools

import jax
import jax.numpy as jnp
from jax import lax
from jax.experimental import pallas as pl
from jax.experimental.pallas import tpu as pltpu
from jax.sharding import PartitionSpec as P

MESH = pl.DeviceIdType.MESH
VMEM = pl.BlockSpec(memory_space=pltpu.VMEM)
bf16, f32 = jnp.bfloat16, jnp.float32


def peer(axis, index):
    return {axis: index}


def greet(axis, targets):
    barrier = pltpu.get_barrier_semaphore()
    for target in targets:
        pl.semaphore_signal(barrier, inc=1, device_id=peer(axis, target), device_id_type=MESH)
    pl.semaphore_wait(barrier, len(targets))


def remote(src, dst, send, recv, axis, target):
    return pltpu.make_async_remote_copy(
        src_ref=src, dst_ref=dst, send_sem=send, recv_sem=recv,
        device_id=peer(axis, target), device_id_type=MESH,
    )


def exchange_kernel(axis, n, same, x_ref, o_ref, send, recv):
    me = lax.axis_index(axis)
    targets = [lax.rem(me + d, n) for d in range(1, n)]
    greet(axis, targets)
    copies = []
    for d in range(1, n):
        src = x_ref if same else x_ref.at[targets[d - 1]]
        copy = remote(src, o_ref.at[me], send.at[d - 1], recv.at[d - 1], axis, targets[d - 1])
        copy.start()
        copies.append(copy)
    o_ref[me] = x_ref[...] if same else x_ref[me]
    for copy in copies:
        copy.wait()


def gather_kernel(axis, n, x_ref, o_ref, send, recv, core_send, core_recv):
    me = lax.axis_index(axis)
    core = lax.rem(me, 2)
    mate = me + 1 - 2 * core
    h = n // 2
    targets = [lax.rem(me + 2 * d, n) for d in range(1, h)]
    greet(axis, [mate] + targets)
    copies = []
    for d in range(1, h):
        copy = remote(x_ref, o_ref.at[me], send.at[d], recv.at[d], axis, targets[d - 1])
        copy.start()
        copies.append(copy)
    passed = [remote(x_ref, o_ref.at[me], core_send.at[0], core_recv.at[0], axis, mate)]
    passed[0].start()
    o_ref[me] = x_ref[...]
    for d in range(1, h):
        source = lax.rem(me + n - 2 * d, n)
        copies[d - 1].wait_recv()
        copy = remote(o_ref.at[source], o_ref.at[source], core_send.at[d], core_recv.at[d], axis, mate)
        copy.start()
        passed.append(copy)
    for copy in copies:
        copy.wait_send()
    for copy in passed:
        copy.wait()


def scatter_kernel(axis, n, x_ref, o_ref, landed, stage, parts, send, recv, core_send, core_recv):
    me = lax.axis_index(axis)
    core = lax.rem(me, 2)
    chip = me // 2
    mate = me + 1 - 2 * core
    h = n // 2
    targets = [lax.rem(me + 2 * d, n) for d in range(1, h)]
    greet(axis, [mate] + targets)
    core_copies = []
    for d in list(range(1, h)) + [0]:
        there = lax.rem(chip + d, h)
        copy = remote(x_ref.at[1 - core, there], landed.at[d], core_send.at[d], core_recv.at[d], axis, mate)
        copy.start()
        core_copies.append(copy)
    copies = []
    for order, d in enumerate(range(1, h)):
        there = lax.rem(chip + d, h)
        core_copies[order].wait_recv()
        stage[d - 1] = (x_ref[core, there].astype(f32) + landed[d].astype(f32)).astype(bf16)
        copy = remote(stage.at[d - 1], parts.at[d - 1], send.at[d - 1], recv.at[d - 1], axis, targets[d - 1])
        copy.start()
        copies.append(copy)
    core_copies[-1].wait_recv()
    total = x_ref[core, chip].astype(f32) + landed[0].astype(f32)
    for d in range(1, h):
        copies[d - 1].wait_recv()
        total = total + parts[d - 1].astype(f32)
    o_ref[...] = total.astype(bf16)
    for copy in copies + core_copies:
        copy.wait_send()


def call(kernel, out, scratch, cid, sent, *args):
    return pl.pallas_call(
        kernel,
        out_shape=out,
        in_specs=[VMEM] * len(args),
        out_specs=jax.tree.map(lambda _: VMEM, out),
        scratch_shapes=scratch,
        compiler_params=pltpu.CompilerParams(collective_id=cid, has_side_effects=True, vmem_limit_bytes=48 * 2**20),
        cost_estimate=pl.CostEstimate(flops=8_000_000_000, bytes_accessed=sent, transcendentals=0),
    )(*args)


def exchange(x, axis, cid, same=False):
    n = lax.axis_size(axis)
    shape = (n,) + x.shape if same else x.shape
    sems = [pltpu.SemaphoreType.DMA((n - 1,))] * 2
    return call(functools.partial(exchange_kernel, axis, n, same), jax.ShapeDtypeStruct(shape, x.dtype), sems, cid, x.nbytes, x)


def gather(x, axis, cid):
    n = lax.axis_size(axis)
    sems = [pltpu.SemaphoreType.DMA((n // 2,))] * 4
    return call(functools.partial(gather_kernel, axis, n), jax.ShapeDtypeStruct((n,) + x.shape, x.dtype), sems, cid, x.nbytes, x)


def scatter(x, axis, cid):
    n = lax.axis_size(axis)
    h, piece = n // 2, x.shape[2:]
    scratch = [pltpu.VMEM((h,) + piece, bf16), pltpu.VMEM((h,) + piece, bf16), pltpu.VMEM((h,) + piece, bf16)]
    scratch += [pltpu.SemaphoreType.DMA((h,))] * 4
    return call(functools.partial(scatter_kernel, axis, n), jax.ShapeDtypeStruct(piece, bf16), scratch, cid, x.nbytes, x)


def lanes(index, width):
    return pl.ds(pl.multiple_of(index * width, width), width)


def chain_kernel(n, zn, chunks, scale, x_ref, v_ref, k_ref, f_ref, o_ref, f_out, landed, stage, parts, c_col, turned, rows,
                 t_out, t_in, spread, n_out, n_in, own_q, rs, zs, ss, ts, ns, gs, fs):
    me, z = lax.axis_index("rows"), lax.axis_index("feat")
    core, chip = lax.rem(me, 2), me // 2
    mate = me + 1 - 2 * core
    h, per = n // 2, n // zn
    nar = t_out.shape[1]
    own = x_ref.shape[0]
    barrier = pltpu.get_barrier_semaphore()
    for d in range(1, n):
        pl.semaphore_signal(barrier, inc=1, device_id={"rows": lax.rem(me + d, n)}, device_id_type=MESH)
    for d in range(1, zn):
        pl.semaphore_signal(barrier, inc=1, device_id={"feat": lax.rem(z + d, zn)}, device_id_type=MESH)
    pl.semaphore_wait(barrier, n + zn - 2)
    ck = f_ref.shape[0] // chunks

    def hop(way, step, unit):
        there = f_out.at[pl.ds(unit * ck, ck), lanes(z - step if way == 0 else z + step, own)]
        src = there if step else f_ref.at[pl.ds(unit * ck, ck)]
        target = lax.rem(z + (1 if way == 0 else zn - 1), zn)
        return remote(src, there, fs[0].at[way, step, unit], fs[1].at[way, step, unit], "feat", target)

    def held(way, step):
        return z >= step if way == 0 else z + step < zn

    def onward(way):
        return z < zn - 1 if way == 0 else z > 0

    def forward(step, some):
        for unit in some:
            for way in (0, 1):
                @pl.when(held(way, step))
                def _():
                    hop(way, step - 1, unit).wait_recv()
                    if step < zn - 1:
                        @pl.when(onward(way))
                        def _():
                            hop(way, step, unit).start()

    every = range(chunks)

    def begin(some):
        for unit in some:
            for way in (0, 1):
                @pl.when(onward(way))
                def _():
                    hop(way, 0, unit).start()

    begin(every[: chunks // 2])
    f_out[:, lanes(z, own)] = f_ref[...]

    pending = []
    core_copies = []
    order = list(range(1, h)) + [0]
    for d in order:
        piece = 2 * lax.rem(chip + d, h) + 1 - core
        copy = remote(x_ref.at[:, lanes(piece, nar)], landed.at[d], rs[0].at[d], rs[1].at[d], "rows", mate)
        copy.start()
        core_copies.append(copy)
    copies = []
    for i, d in enumerate(order):
        piece = 2 * lax.rem(chip + d, h) + core
        core_copies[i].wait_recv()
        both = x_ref[:, lanes(piece, nar)].astype(f32) + landed[d].astype(f32)
        if d:
            stage[d] = both.astype(bf16)
            copy = remote(stage.at[d], parts.at[d], rs[2].at[d], rs[3].at[d], "rows", lax.rem(me + 2 * d, n))
            copy.start()
            copies.append(copy)
    for d in range(1, h):
        copies[d - 1].wait_recv()
        both = both + parts[d].astype(f32)
    c_col[z] = both.astype(bf16)
    pending += core_copies + copies

    def pass_tiles(block):
        for i in range(per):
            s = block * per + i
            off = lax.rem(s - me + n, n)

            @pl.when(off != 0)
            def _():
                remote(c_col.at[block, pl.ds(i * nar, nar)], turned.at[me], ss[0].at[off - 1], ss[1].at[off - 1], "rows", s).start()

            @pl.when(off == 0)
            def _():
                turned[me] = c_col[block, pl.ds(i * nar, nar)]

    z_copies = []
    for d in range(1, zn):
        copy = remote(c_col.at[z], c_col.at[z], zs[0].at[d - 1], zs[1].at[d - 1], "feat", lax.rem(z + d, zn))
        copy.start()
        z_copies.append(copy)
    begin(every[chunks // 2 :])
    pass_tiles(z)
    for d in range(1, zn):
        z_copies[d - 1].wait_recv()
        pass_tiles(lax.rem(z + zn - d, zn))
    pending += z_copies
    forward(1, every)

    def add_rows(source):
        inner = c_col[source // per, pl.ds(pl.multiple_of(lax.rem(source, per) * nar, nar), nar)]
        both = 0.5 * (turned[source].astype(f32) + inner.astype(f32).T)
        rows[:, lanes(source, nar)] = both.astype(bf16)

    for d in range(n):
        source = lax.rem(me + n - d, n)
        if d:
            copy = remote(c_col.at[0, pl.ds(0, nar)], turned.at[source], ss[0].at[d - 1], ss[1].at[d - 1], "rows", lax.rem(me + d, n))
            copy.wait_recv()
            pending.append(copy)
        add_rows(source)

    def swap(make, outs, ins, sems):
        copies = []
        for d in list(range(1, n)) + [0]:
            s = lax.rem(me + d, n)
            piece = make(s).astype(bf16)
            if d:
                outs[s] = piece
                copy = remote(outs.at[s], ins.at[me], sems[0].at[d - 1], sems[1].at[d - 1], "rows", s)
                copy.start()
                copies.append(copy)
            else:
                ins[me] = piece
        return copies

    half = zn // 2
    for step in range(2, half):
        forward(step, every)
    t_copies = swap(lambda s: jnp.dot(rows[...], v_ref[s], preferred_element_type=f32), t_out, t_in, ts)
    for d in range(n):
        source = lax.rem(me + n - d, n)
        if d:
            t_copies[d - 1].wait_recv()
        spread[:, lanes(source, nar)] = t_in[source].astype(f32).T.astype(bf16)
    pending += t_copies
    if half > 1:
        forward(half, every[: chunks // 2])
    for q in range(n):
        block = jnp.dot(spread[...], v_ref[q], preferred_element_type=f32)
        rows[:, pl.ds(q * nar, nar)] = (k_ref[:, pl.ds(q * nar, nar)] * block).astype(bf16)

    def back(s):
        total = None
        for q in range(n):
            term = lax.dot_general(
                rows[:, pl.ds(q * nar, nar)], v_ref[q, pl.ds(pl.multiple_of(s * nar, nar), nar)],
                (((1,), (1,)), ((), ())), preferred_element_type=f32,
            )
            total = term if total is None else total + term
        return total

    n_copies = swap(back, n_out, n_in, ns)
    pending += n_copies
    if half > 1:
        forward(half, every[chunks // 2 :])
    total = None
    for d in range(n):
        source = lax.rem(me + n - d, n)
        if d:
            n_copies[d - 1].wait_recv()
        left = v_ref[source, pl.ds(pl.multiple_of(z * own, own), own)]
        term = jnp.dot(left, n_in[source], preferred_element_type=f32)
        total = term if total is None else total + term
    own_q[...] = (scale * total).astype(bf16)

    copies, passed = [], []
    mine = o_ref.at[:, lanes(me, nar)]
    for d in range(1, h):
        copy = remote(own_q, mine, gs[0].at[d], gs[1].at[d], "rows", lax.rem(me + 2 * d, n))
        copy.start()
        copies.append(copy)
    passed.append(remote(own_q, mine, gs[2].at[0], gs[3].at[0], "rows", mate))
    passed[0].start()
    o_ref[:, lanes(me, nar)] = own_q[...]
    for d in range(1, h):
        there = o_ref.at[:, lanes(lax.rem(me + n - 2 * d, n), nar)]
        copies[d - 1].wait_recv()
        copy = remote(there, there, gs[2].at[d], gs[3].at[d], "rows", mate)
        copy.start()
        passed.append(copy)
    for step in range(max(half, 1) + 1, zn):
        forward(step, every)
    for copy in passed:
        copy.wait()
    for copy in copies + pending:
        copy.wait_send()
    for step in range(zn - 1):
        for unit in every:
            for way in (0, 1):
                @pl.when(jnp.logical_and(held(way, step), onward(way)))
                def _():
                    hop(way, step, unit).wait_send()


def chain(part, v_pieces, kernel_rows, x, row_count):
    n, zn = lax.axis_size("rows"), lax.axis_size("feat")
    own, d_all = part.shape
    nar, h = d_all // n, n // 2
    tile, square = (h, own, nar), (n, nar, nar)
    dma = pltpu.SemaphoreType.DMA
    scratch = [pltpu.VMEM(tile, bf16)] * 3 + [pltpu.VMEM((zn, own, nar), bf16), pltpu.VMEM(square, bf16)]
    scratch += [pltpu.VMEM((nar, d_all), bf16), pltpu.VMEM(square, bf16), pltpu.VMEM(square, bf16)]
    scratch += [pltpu.VMEM((nar, d_all), bf16), pltpu.VMEM(square, bf16), pltpu.VMEM(square, bf16)]
    scratch += [pltpu.VMEM((own, nar), bf16)]
    scratch += [[dma((h,))] * 4, [dma((zn - 1,))] * 2, [dma((n - 1,))] * 2, [dma((n - 1,))] * 2]
    chunks = 4
    scratch += [[dma((n - 1,))] * 2, [dma((h,))] * 4, [dma((2, zn - 1, chunks))] * 2]
    kernel = functools.partial(chain_kernel, n, zn, chunks, 2.0 / row_count)
    out = (jax.ShapeDtypeStruct((own, d_all), bf16), jax.ShapeDtypeStruct((x.shape[0], own * zn), bf16))
    return call(kernel, out, scratch, 9, 8 * part.nbytes, part, v_pieces, kernel_rows, x)


def front_kernel(n, zn, chunks, g_ref, v_ref, g_out, v_out, send, recv, near, far, mate_send, mate_recv):
    me, z = lax.axis_index("rows"), lax.axis_index("feat")
    core = lax.rem(me, 2)
    mate = me + 1 - 2 * core
    h = n // 2
    own, ck = v_ref.shape[0], g_ref.shape[0] // chunks
    units = chunks + 1
    peers = [lax.rem(me + 2 * d, n) for d in range(1, h)]
    barrier = pltpu.get_barrier_semaphore()
    for target in [mate] + peers:
        pl.semaphore_signal(barrier, inc=1, device_id={"rows": target}, device_id_type=MESH)
    for d in range(1, zn):
        pl.semaphore_signal(barrier, inc=1, device_id={"feat": lax.rem(z + d, zn)}, device_id_type=MESH)
    pl.semaphore_wait(barrier, h + zn - 1)

    def there(block, unit):
        if unit == 0:
            return v_out.at[me, pl.ds(pl.multiple_of(block * own, own), own)]
        return g_out.at[pl.ds((unit - 1) * ck, ck), lanes(block, own)]

    def hop(way, step, unit):
        block = z - step if way == 0 else z + step
        if step == 0:
            src = v_ref if unit == 0 else g_ref.at[pl.ds((unit - 1) * ck, ck)]
        else:
            src = there(block, unit)
        target = lax.rem(z + (1 if way == 0 else zn - 1), zn)
        return remote(src, there(block, unit), send.at[way, step, unit], recv.at[way, step, unit], "feat", target)

    def held(way, step):
        return z >= step if way == 0 else z + step < zn

    def onward(way):
        return z < zn - 1 if way == 0 else z > 0

    def spread(block, d, fresh=False):
        src = v_ref if fresh else there(block, 0)
        return remote(src, there(block, 0), near.at[block, d], far.at[block, d], "rows", peers[d - 1])

    def to_mate(block, d, fresh=False):
        source = lax.rem(me + n - 2 * d, n) if d else me
        ref = v_out.at[source, pl.ds(pl.multiple_of(block * own, own), own)]
        src = v_ref if fresh else ref
        return remote(src, ref, mate_send.at[block, d], mate_recv.at[block, d], "rows", mate)

    def spread_all(block, fresh=False):
        for d in range(1, h):
            spread(block, d, fresh).start()
        to_mate(block, 0, fresh).start()

    def pass_mate(block):
        for d in range(1, h):
            spread(block, d).wait_recv()
            to_mate(block, d).start()

    def each(step, what):
        if step == 0:
            what(z)
            return
        for way in (0, 1):
            @pl.when(held(way, step))
            def _():
                what(z - step if way == 0 else z + step)

    for unit in range(units):
        for way in (0, 1):
            @pl.when(onward(way))
            def _():
                hop(way, 0, unit).start()
    spread_all(z, True)
    v_out[me, pl.ds(pl.multiple_of(z * own, own), own)] = v_ref[...]
    g_out[:, lanes(z, own)] = g_ref[...]
    for step in range(1, zn):
        for unit in range(units):
            for way in (0, 1):
                @pl.when(held(way, step))
                def _():
                    hop(way, step - 1, unit).wait_recv()
                    if step < zn - 1:
                        @pl.when(onward(way))
                        def _():
                            hop(way, step, unit).start()
                    if unit == 0:
                        spread_all(z - step if way == 0 else z + step)
        each(step - 1, pass_mate)
    each(zn - 1, pass_mate)

    def finish(block):
        for d in range(1, h):
            spread(block, d).wait_send()
        for d in range(h):
            to_mate(block, d).wait()

    for step in range(zn):
        each(step, finish)
    for step in range(zn - 1):
        for unit in range(units):
            for way in (0, 1):
                @pl.when(jnp.logical_and(held(way, step), onward(way)))
                def _():
                    hop(way, step, unit).wait_send()


def front(g, v):
    n, zn = lax.axis_size("rows"), lax.axis_size("feat")
    tok, own = g.shape
    chunks = 4
    dma = pltpu.SemaphoreType.DMA
    out = (jax.ShapeDtypeStruct((tok, own * zn), bf16), jax.ShapeDtypeStruct((n, own * zn, v.shape[1]), bf16))
    scratch = [dma((2, zn - 1, chunks + 1))] * 2 + [dma((zn, n // 2))] * 4
    kernel = functools.partial(front_kernel, n, zn, chunks)
    return call(kernel, out, scratch, 10, zn * g.nbytes, g, v)


def divided(lam_row, lam_col, first_row):
    on_diag = (
        (first_row + jnp.arange(lam_row.shape[0], dtype=jnp.int32))[:, None]
        == jnp.arange(lam_col.shape[0], dtype=jnp.int32)[None, :]
    )
    root_row = lam_row ** (-0.5)
    root_col = lam_col ** (-0.5)
    gaps_lam = lam_row[:, None] - lam_col[None, :]
    safe_gap = jnp.where(on_diag, jnp.ones_like(gaps_lam), gaps_lam)
    off_diag = (root_row[:, None] - root_col[None, :]) / safe_gap
    diag_vals = -0.5 * lam_row[:, None] ** (-1.5) + jnp.zeros_like(gaps_lam)
    return jnp.where(on_diag, diag_vals, off_diag)


def dot(a, b, ca, cb):
    return lax.dot_general(a, b, (((ca,), (cb,)), ((), ())), preferred_element_type=f32)


def chain_by_calls(part, v_pieces, kernel_rows, row_count):
    n = lax.axis_size("rows")
    own, d_all = part.shape
    nar = d_all // n
    v_all = v_pieces.transpose(1, 0, 2).reshape(d_all, d_all)
    part = part.reshape(own, n // 2, 2, nar).transpose(2, 1, 0, 3)
    tile = scatter(part, "rows", 3)
    c_col = exchange(tile, "feat", 4, same=True).reshape(n, nar, nar)
    turned = exchange(c_col, "rows", 5)
    both = 0.5 * (c_col.astype(f32) + turned.transpose(0, 2, 1).astype(f32))
    half = dot(v_all, both.reshape(d_all, nar).astype(bf16), 0, 0).astype(bf16)
    half = exchange(half.reshape(n, nar, nar), "rows", 6)
    rotated = dot(half.transpose(1, 0, 2).reshape(nar, d_all), v_all, 1, 0)
    back = dot((kernel_rows * rotated).astype(bf16), v_all, 1, 1).astype(bf16)
    back = exchange(back.reshape(nar, n, nar).transpose(1, 0, 2), "rows", 7).reshape(d_all, nar)
    v_own = lax.dynamic_slice_in_dim(v_all, lax.axis_index("feat") * own, own)
    sens = (2.0 / row_count * dot(v_own, back, 1, 0)).astype(bf16)
    return gather(sens, "rows", 8).transpose(1, 0, 2).reshape(own, d_all)


def local(features, grad_out, eigvecs, eigvals, whiten):
    tok_rows, own = features.shape
    n = lax.axis_size("rows")
    d_all = eigvals.shape[0]
    nar = d_all // n
    row_count = tok_rows * n
    me = lax.axis_index("rows")

    sums = jnp.stack([jnp.sum(features, axis=0, dtype=f32), jnp.sum(grad_out, axis=0, dtype=f32)])
    sums = jnp.pad(sums, ((0, 6), (0, 0)))
    means = jnp.sum(gather(sums, "rows", 1), axis=0) / row_count
    xc = (features.astype(f32) - means[0]).astype(bf16)
    gc = (grad_out.astype(f32) - means[1]).astype(bf16)
    g_all, v_pieces = front(gc, eigvecs.astype(bf16))
    first = me * nar
    lam_row = lax.dynamic_slice_in_dim(eigvals, first, nar)
    kernel_rows = divided(lam_row, eigvals, first)
    part = dot(xc, g_all, 0, 0).astype(bf16)
    if nar % 128 == 0:
        sens, x_all = chain(part, v_pieces, kernel_rows, xc, row_count)
    else:
        x_all = lax.all_gather(xc, "feat", axis=1, tiled=True)
        sens = chain_by_calls(part, v_pieces, kernel_rows, row_count)
    grad_in = dot(g_all, whiten, 1, 0) + dot(x_all, sens, 1, 1)
    return grad_in.astype(bf16)


def solution(mesh):
    in_specs = (P("rows", "feat"), P("rows", "feat"), P("feat", "rows"), P(), P(None, "feat"))
    out_specs = P("rows", "feat")
    return jax.shard_map(local, mesh=mesh, in_specs=in_specs, out_specs=out_specs, check_vma=False)
```
